32 devices in a mesh: leaf: 8 (over y, x, core), group: 4 (over z).
Axes of the slice: x: 2, y: 2, z: 4, core: 2. Of those that a mesh axis runs over, the one named last changes fastest.
Arguments:
- coefficients: float32 [4, 4096, 512], P('group', 'leaf'), may hold values from -6 to 6
- labels: float32 [4, 4096, 512], P('group', 'leaf'), may hold values from -6 to 6
- near_kernel: float32 [4, 4096, 3072], P('group', 'leaf'), may hold values from -0.109375 to 0.109375
- basis: float32 [4, 4096, 256], P('group', 'leaf'), may hold values from -0.1875 to 0.1875
- transfer: float32 [4, 1024, 256], P('group', 'leaf'), may hold values from -0.375 to 0.375
- coupling: float32 [4, 256, 1024], P('group', 'leaf'), may hold values from -0.1875 to 0.1875
- near_lists: int32 [4, 4, 3], P('group'), may hold values from 0 to 3, as said below
- ridge: float32 [1], replicated, may hold values from 0.5 to 2
Outputs:
- residual: float32 [4, 4096, 512], P('group', 'leaf')
The draws below stay inside these ranges and needn't reach their ends.
Inputs may be any that keep to these rules, and one draw needn't show every extreme that they name: `near_lists`: entry 0 of each leaf's list is the leaf itself; in each group the leaves lie on one cycle through all 4 leaves, and entries 1 and 2 of a leaf's list are its two neighbours on that cycle.
All inputs are finite; a program needn't handle non-finite values.
Results may differ from the reference program's by a relative error of at most 0.0011.
Values may be sent and summed in bfloat16 or wider, within the bound.
No kernel may reach another device: no remote copies, remote signals or barrier semaphores. Data moves between devices by JAX's collectives and lax.ppermute only.
A program may use at most 64 MiB of HBM per device.

```python
import math
import jax
import jax.numpy as jnp
from jax import lax

LEAF = 1024
RANK = 256
COLS = 512
LPG = 4
NEAR = 3
GROUPS = 4
GROUP_ROWS = 4096


def draw_near_lists(key, part):
    group_keys = jax.random.split(jax.random.fold_in(key, 17), GROUPS)
    counting = jnp.arange(LPG, dtype=jnp.int32)

    def one_group(group_key):
        order = jax.random.permutation(group_key, LPG).astype(jnp.int32)
        place = jnp.zeros((LPG,), jnp.int32).at[order].set(counting)
        successor = order[(place + 1) % LPG]
        predecessor = order[(place + LPG - 1) % LPG]
        return jnp.stack([counting, successor, predecessor], axis=1)
    return jax.vmap(one_group)(group_keys).astype(jnp.int32)


def shard_levels(stream_key, dims, cuts, smallest, largest):
    def one(dim, parts):
        draws = jax.random.uniform(jax.random.fold_in(jax.random.fold_in(stream_key, 6), dim), (parts,), jnp.float32, smallest / len(cuts), largest / len(cuts))
        return jnp.repeat(jnp.exp(draws), dims[dim] // parts).reshape((-1,) + (1,) * (len(dims) - dim - 1))

    factor_of = one(*cuts[0])
    for cut in cuts[1:]:
        factor_of = factor_of * one(*cut)
    return factor_of


def noise(stream_key, dims, spread, reach, cuts=(), kind=jnp.bfloat16):
    array = jax.random.normal(stream_key, dims, jnp.float32) * spread
    if len(cuts) > 0:
        array = shard_levels(stream_key, dims, cuts, -0.22, 0.18) * array
    return jnp.clip(array, min=-reach, max=reach).astype(kind)


def setup_inputs(seed: int = 0) -> dict:
    splits = jax.random.split(jax.random.key(seed), 9)
    return {
        "coefficients": noise(splits[0], (GROUPS, GROUP_ROWS, COLS), 1.0, 6.0, ((0, 4), (1, 8)), jnp.float32),
        "labels": noise(splits[1], (GROUPS, GROUP_ROWS, COLS), 1.0, 6.0, ((0, 4), (1, 8)), jnp.float32),
        "near_kernel": noise(splits[2], (GROUPS, GROUP_ROWS, NEAR * LEAF), (NEAR * LEAF) ** -0.5, 0.109375, ((0, 4), (1, 8)), jnp.float32),
        "basis": noise(splits[3], (GROUPS, GROUP_ROWS, RANK), LEAF ** -0.5, 0.1875, ((0, 4), (1, 8)), jnp.float32),
        "transfer": noise(splits[4], (GROUPS, LPG * RANK, RANK), RANK ** -0.5, 0.375, ((0, 4), (1, 8)), jnp.float32),
        "coupling": noise(splits[5], (GROUPS, RANK, GROUPS * RANK), (GROUPS * RANK) ** -0.5, 0.1875, ((0, 4), (1, 8)), jnp.float32),
        "near_lists": draw_near_lists(jax.random.fold_in(splits[8], 71), 0),
        "ridge": jnp.clip(jnp.exp(jax.random.uniform(splits[7], (1,), jnp.float32, math.log(0.5), math.log(2.0))), 0.5, 2.0),
    }


def reference(coefficients, labels, near_kernel, basis, transfer, coupling, near_lists, ridge):
    highest = lax.Precision.HIGHEST
    groups = coefficients.shape[0]
    leaves = coefficients.reshape(groups, LPG, LEAF, COLS)
    group_index = jnp.arange(groups, dtype=jnp.int32)[:, None, None]
    nearby = leaves[group_index, near_lists]
    kernel_blocks = near_kernel.reshape(groups, LPG, LEAF, NEAR, LEAF)
    near = jnp.einsum("giasb,gisbc->giac", kernel_blocks, nearby, precision=highest)
    leaf_basis = basis.reshape(groups, LPG, LEAF, RANK)
    leaf_coef = jnp.einsum("giar,giac->girc", leaf_basis, leaves, precision=highest)
    transfers = transfer.reshape(groups, LPG, RANK, RANK)
    group_coef = jnp.einsum("girs,girc->gsc", transfers, leaf_coef, precision=highest)
    group_round = lax.optimization_barrier(group_coef.astype(jnp.bfloat16)).astype(jnp.float32)
    stacked = group_round.reshape(groups * RANK, COLS)
    coarse = jnp.einsum("gsk,kc->gsc", coupling, stacked, precision=highest)
    downward = jnp.einsum("girs,gsc->girc", transfers, coarse, precision=highest)
    far = jnp.einsum("giar,girc->giac", leaf_basis, downward, precision=highest)
    total = near + far + ridge[0] * leaves
    result = labels.reshape(groups, LPG, LEAF, COLS) - total
    return result.reshape(groups, LPG * LEAF, COLS)
```

```python
import functools
import jax
import jax.numpy as jnp
from jax import lax
from jax.experimental import pallas as pl
from jax.experimental.pallas import tpu as pltpu
from jax.sharding import PartitionSpec as P

F32 = jnp.float32
BF16 = jnp.bfloat16
VMEM = pl.BlockSpec(memory_space=pltpu.VMEM)
SMEM = pl.BlockSpec(memory_space=pltpu.SMEM)

NN = (((1,), (0,)), ((), ()))
NT = (((1,), (1,)), ((), ()))
TN = (((0,), (0,)), ((), ()))


def dot(left, right, dims):
    return lax.dot_general(left, right, dims, preferred_element_type=F32)


def halves(value):
    high = value.astype(BF16)
    return high, (value - high.astype(F32)).astype(BF16)


def dot3(left, right, dims):
    left_high, left_low = halves(left)
    right_high, right_low = halves(right)
    return (
        dot(left_high, right_high, dims)
        + dot(left_high, right_low, dims)
        + dot(left_low, right_high, dims)
    )


def call(body, outs, *operands, name, scratch=(), aliases={}, scalars=0, flops=0):
    return pl.pallas_call(
        body,
        out_shape=outs,
        in_specs=[SMEM] * scalars + [VMEM] * (len(operands) - scalars),
        out_specs=jax.tree.map(lambda _: VMEM, outs),
        scratch_shapes=list(scratch),
        input_output_aliases=aliases,
        name=name,
        cost_estimate=pl.CostEstimate(flops=flops, bytes_accessed=0, transcendentals=0),
    )(*operands)


def shape(dims, kind=F32):
    return jax.ShapeDtypeStruct(dims, kind)


def split_kernel(source, high, low):
    high[...], low[...] = halves(source[...])


def own_kernel(split, index, ridge, high, low, labels, *refs):
    pieces, total = refs[:-1], refs[-1]
    rows = pieces[0].shape[0]
    result = labels[...] - ridge[0] * pieces[0][...]
    for offset in range(split):
        columns = pl.ds(pl.multiple_of(index[0, offset] * rows, 128), rows)
        piece_high, piece_low = halves(pieces[offset][...])
        result -= (
            dot(high[:, columns], piece_high, NN)
            + dot(low[:, columns], piece_high, NN)
            + dot(high[:, columns], piece_low, NN)
        )
    total[...] = result


def near_update(split, index, high, low, groups, total):
    for leaf_offset, side, pieces in groups:
        rows, width = pieces[0].shape
        target = pl.ds(side * width, width)

        @pl.when(index[leaf_offset, split] > 0)
        def _():
            result = total[:, target]
            for offset in range(split):
                columns = pl.ds(pl.multiple_of(index[leaf_offset, offset] * rows, 128), rows)
                piece = pieces[offset][...]
                result -= dot(high[:, columns], piece, NN) + dot(low[:, columns], piece, NN)
            total[:, target] = result


def near_kernel_body(split, plan, index, high, low, *refs):
    pieces, start, total = refs[:-2], refs[-2], refs[-1]
    total[...] = start[...]
    groups = [
        (leaf_offset, side, pieces[k * split : (k + 1) * split])
        for k, (leaf_offset, side) in enumerate(plan)
    ]
    near_update(split, index, high, low, groups, total)


def gather_rows(place, pieces, whole):
    for k, piece in enumerate(pieces):
        rows = piece.shape[0]
        whole[pl.ds(pl.multiple_of(place[k] * rows, 8), rows), :] = piece[...]


def contribution_kernel(split, place, half, coefficients, basis, *refs):
    pieces, (give, keep, transfer, whole) = refs[:split], refs[split:]
    gather_rows(place, pieces, transfer)
    leaf = dot3(coefficients[...], basis[...], TN)
    whole[...] = dot3(leaf, transfer[...], NN)
    size = give.shape[0]
    keep[...] = whole[pl.ds(pl.multiple_of(half[0] * size, 8), size), :]
    give[...] = whole[pl.ds(pl.multiple_of((1 - half[0]) * size, 8), size), :]


def parts_kernel(place, keep, received, *refs):
    parts, whole = refs[:-1], refs[-1]
    whole[...] = keep[...] + received[...]
    for k, part in enumerate(parts):
        size = part.shape[0]
        part[...] = whole[pl.ds(pl.multiple_of(place[k] * size, 8), size), :]


def coupling_kernel(count, place, *refs):
    pieces, (high, low, whole) = refs[:count], refs[count:]
    gather_rows(place, pieces, whole)
    high[...], low[...] = halves(whole[...])


def coarse_kernel(count, place, high, low, *refs):
    pieces, out = refs[:count], refs[count]
    result = None
    for k, piece in enumerate(pieces):
        rank = piece.shape[1]
        columns = pl.ds(pl.multiple_of(place[k] * rank, 128), rank)
        value = piece[...]
        part = dot(value, high[:, columns], NT) + dot(value, low[:, columns], NT)
        result = part if result is None else result + part
    out[...] = result


def final_kernel(split, plan, count, index, leaf_place, coarse_place, high, low, basis, *refs):
    transfer_pieces, refs = refs[:split], refs[split:]
    coarse_pieces, refs = refs[:count], refs[count:]
    near_pieces, (start, total, transfer, coarse) = refs[:-4], refs[-4:]
    gather_rows(leaf_place, transfer_pieces, transfer)
    gather_rows(coarse_place, coarse_pieces, coarse)
    downward = dot3(coarse[...], transfer[...], NT)
    total[...] = start[...] - dot3(basis[...], downward, NT)
    groups = [
        (leaf_offset, side, near_pieces[k * split : (k + 1) * split])
        for k, (leaf_offset, side) in enumerate(plan)
    ]
    near_update(split, index, high, low, groups, total)


def shards(coefficients, labels, near_kernel, basis, transfer, coupling, near_lists, ridge):
    own, labels, basis = coefficients[0], labels[0], basis[0]
    kernel, transfer, coupling, lists = near_kernel[0], transfer[0], coupling[0], near_lists[0]
    leaves, list_length = lists.shape
    devices, groups = lax.axis_size("leaf"), lax.axis_size("group")
    split = devices // leaves
    levels = split.bit_length() - 1
    rows, columns = own.shape
    rank = basis.shape[1]
    position, group = lax.axis_index("leaf"), lax.axis_index("group")
    leaf, sub = position // split, position % split
    offsets = jnp.arange(split, dtype=jnp.int32)

    def moved(value, mask):
        return lax.ppermute(value, "leaf", [(i, i ^ mask) for i in range(devices)])

    def across(value, leaf_offset):
        return moved(value, leaf_offset * split)

    def within(value):
        pieces = [value]
        for level in range(levels):
            pieces += [moved(piece, 1 << level) for piece in pieces]
        return pieces

    chosen = lax.dynamic_index_in_dim(lists, leaf, 0, keepdims=False)
    others = leaf ^ jnp.arange(leaves, dtype=jnp.int32)
    match = (others[:, None] == chosen[None, :]).astype(jnp.int32)
    block = jnp.sum(match * jnp.arange(list_length, dtype=jnp.int32)[None, :], axis=1)
    index = jnp.concatenate(
        [block[:, None] * split + (sub ^ offsets)[None, :], jnp.sum(match, axis=1)[:, None]], axis=1
    )
    leaf_place = sub ^ offsets

    width = columns // 2
    side0, side1 = own[:, :width].astype(BF16), own[:, width:].astype(BF16)
    x0, y1 = across(side0, 1), across(side1, 2)

    transfer_pieces = within(transfer)
    half = (sub & 1).reshape(1)
    give, keep = call(
        functools.partial(contribution_kernel, split),
        [shape((columns // 2, rank))] * 2,
        leaf_place, half, own, basis, *transfer_pieces,
        name="contribution", scalars=2,
        scratch=[pltpu.VMEM((rank, rank), F32), pltpu.VMEM((columns, rank), F32)],
        flops=6 * columns * rank * (rows + rank),
    )
    received = moved(give, 1)
    start = (sub & 1) * (columns // 2)
    for level in range(1, levels):
        size = keep.shape[0] // 2
        value = keep + received
        upper = sub >> level & 1
        keep = lax.dynamic_slice_in_dim(value, upper * size, size, 0)
        give = lax.dynamic_slice_in_dim(value, (1 - upper) * size, size, 0)
        received = moved(give, 1 << level)
        start = start + upper * size
    size = keep.shape[0] // leaves
    parts = call(
        parts_kernel, [shape((size, rank))] * leaves, others, keep, received,
        name="parts", scalars=1, scratch=[pltpu.VMEM(keep.shape, F32)], flops=keep.size * 8,
    )
    group_coef = parts[0]
    for leaf_offset in range(1, leaves):
        group_coef = group_coef + across(parts[leaf_offset], leaf_offset)
    group_round = group_coef.astype(BF16)

    coupling_pieces = []
    for leaf_offset in range(leaves):
        piece = across(coupling, leaf_offset) if leaf_offset else coupling
        coupling_pieces += within(piece)
    place = (others[:, None] * split + leaf_place[None, :]).reshape(-1)
    coupling_high, coupling_low = call(
        functools.partial(coupling_kernel, devices),
        [shape((rank, groups * rank), BF16)] * 2, place, *coupling_pieces,
        name="coupling", scalars=1, scratch=[pltpu.VMEM((rank, groups * rank), F32)],
        flops=rank * groups * rank * 4,
    )
    rounds = [group_round]
    for shift in range(1, groups):
        rounds.append(lax.ppermute(group_round, "group", [(i, (i + shift) % groups) for i in range(groups)]))
    sources = (group + groups - jnp.arange(groups, dtype=jnp.int32)) % groups
    coarse = call(
        functools.partial(coarse_kernel, groups), shape((size, rank)),
        sources, coupling_high, coupling_low, *rounds,
        name="coarse", scalars=1, flops=4 * size * rank * rank * groups,
    )
    coarse_pieces = []
    for leaf_offset in range(leaves):
        coarse_pieces += within(across(coarse, leaf_offset) if leaf_offset else coarse)
    starts = []
    for offset in range(split):
        other = sub ^ offset
        begin = other * 0
        for level in range(levels):
            begin = begin + (other >> level & 1) * (split >> (level + 1))
        starts.append(begin)
    coarse_place = (jnp.stack(starts)[None, :] * leaves + others[:, None]).reshape(-1)

    high, low = pl.pallas_call(
        split_kernel,
        grid=(2 * list_length,),
        in_specs=[pl.BlockSpec((rows, kernel.shape[1] // (2 * list_length)), lambda k: (0, k))],
        out_specs=[pl.BlockSpec((rows, kernel.shape[1] // (2 * list_length)), lambda k: (0, k))] * 2,
        out_shape=[shape(kernel.shape, BF16)] * 2,
        name="split",
    )(kernel)
    near_flops = 4 * rows * rows * split * columns
    total = call(
        functools.partial(own_kernel, split), shape((rows, columns)),
        index, ridge, high, low, labels, *within(own),
        name="own", scalars=2, flops=6 * rows * rows * split * columns,
    )

    def near(total, plan, values, name):
        pieces = [piece for value in values for piece in within(value)]
        return call(
            functools.partial(near_kernel_body, split, plan), shape((rows, columns)),
            index, high, low, *pieces, total,
            name=name, scalars=1, aliases={3 + len(pieces): 0}, flops=near_flops,
        )

    total = near(total, ((1, 0), (2, 1)), (x0, y1), "near_first")
    x1, y0 = across(side1, 1), across(side0, 2)
    total = near(total, ((1, 1), (2, 0)), (x1, y0), "near_second")
    d0, d1 = across(x0, 2), across(y1, 1)
    last = [piece for value in (d0, d1) for piece in within(value)]
    plan = ((3, 0), (3, 1))
    count = devices
    operands = [
        index, leaf_place, coarse_place, high, low, basis,
        *transfer_pieces, *coarse_pieces, *last, total,
    ]
    result = call(
        functools.partial(final_kernel, split, plan, count), shape((rows, columns)), *operands,
        name="final", scalars=3, aliases={len(operands) - 1: 0},
        scratch=[pltpu.VMEM((rank, rank), F32), pltpu.VMEM((columns, rank), F32)],
        flops=near_flops + 6 * columns * rank * (rank + rows),
    )
    return result[None]


def solution(mesh):
    return jax.shard_map(
        shards,
        mesh=mesh,
        in_specs=(
            P("group", "leaf", None),
            P("group", "leaf", None),
            P("group", "leaf", None),
            P("group", "leaf", None),
            P("group", "leaf", None),
            P("group", "leaf", None),
            P("group", None, None),
            P(),
        ),
        out_specs=P("group", "leaf", None),
        check_vma=False,
    )
```
